16 devices in a mesh: data: 4 (over z, y), tp: 4 (over x, core).
Axes of the slice: x: 2, y: 2, z: 2, core: 2. Of those that a mesh axis runs over, the one named last changes fastest.
Arguments:
- x: bfloat16 [1024, 32768], P('data', 'tp'), parts along dimension 0
- w: bfloat16 [32768, 8192], P('tp')
- lengths: int32 [16], P('data'), parts along dimension 0
Outputs:
- output: bfloat16 [1024, 8192], P('data'), parts along dimension 0
There are 4 independent parts. The reference program is written for one: setup_inputs(seed, part) draws one part's arguments, and reference() takes and returns one part's arrays. A program takes and returns all parts, laid end to end along the dimension named above; an argument that names none is the same for every part.
All inputs are finite; a program needn't handle non-finite values.
Results may differ from the reference program's by a relative error of at most 0.001.
Values are sent between devices in bfloat16 or wider.
A program may use at most 1 GiB of HBM per device.

```python
import jax
import jax.numpy as jnp

D = 8192
FF = 32768
TOKENS = 256
SEQS = 4
SEQ_LEN = TOKENS // SEQS


def draw_lengths(key_len):
    key_draw, key_perm = jax.random.split(key_len)
    lengths = jax.random.randint(key_draw, (SEQS,), 1, SEQ_LEN + 1, dtype=jnp.int32)
    slot_order = jax.random.permutation(key_perm, SEQS)
    lengths = lengths.at[slot_order[0]].set(SEQ_LEN)
    lengths = lengths.at[slot_order[1]].set(1)
    return lengths


def setup_inputs(seed: int = 0, part: int = 0) -> dict:
    key = jax.random.key(seed)
    key_x, key_w, key_len = jax.random.split(key, 3)
    tok_acts = jax.random.normal(jax.random.fold_in(key_x, part), (TOKENS, FF), jnp.float32)
    weight = jax.random.normal(key_w, (FF, D), jnp.float32) * (FF ** -0.5)
    lengths = draw_lengths(jax.random.fold_in(key_len, part))
    return {"x": tok_acts.astype(jnp.bfloat16), "w": weight.astype(jnp.bfloat16), "lengths": lengths}


def reference(x, w, lengths):
    seq_len = x.shape[0] // lengths.shape[0]
    valid = (jnp.arange(seq_len, dtype=jnp.int32)[None, :] < lengths[:, None]).reshape(-1)
    full_sum = jnp.dot(x, w, preferred_element_type=jnp.float32)
    return jnp.where(valid[:, None], full_sum, 0.0).astype(jnp.bfloat16)
```

```python
import functools

import jax
import jax.numpy as jnp
from jax import lax
from jax.experimental import pallas as pl
from jax.experimental.pallas import tpu as pltpu
from jax.sharding import PartitionSpec as P

MESH = pl.DeviceIdType.MESH
ROWS = 208
CN = 512
KB = 2048
SLOTS = 8
LAG_B, LAG_C, LAG_D = 1, 3, 5


def row_targets(len_ref, shape, axis, seq_len):
    row = lax.broadcasted_iota(jnp.int32, shape, axis)
    target = jnp.full(shape, -1, jnp.int32)
    start = jnp.int32(0)
    for s in range(len_ref.shape[0]):
        inside = (row >= s * seq_len) & (row < s * seq_len + len_ref[s])
        target = jnp.where(inside, row - s * seq_len + start, target)
        start = start + len_ref[s]
    return target


def matmul_kernel(len_ref, x_hbm, w_hbm, y_ref, x_buf, xc, w_buf, part, d2d_in, ici_in,
                  x_sem, w_sem, d2d_s, d2d_r, ici_s, ici_r, yx_s, yx_r, yp_s, yp_r, yf_s, yf_r):
    tokens, depth = x_hbm.shape
    rows = xc.shape[0]
    width = w_hbm.shape[1]
    nc, nk = width // CN, depth // KB
    total = nc * nk
    seq_len = tokens // len_ref.shape[0]
    tp = lax.axis_index("tp")
    me_x, me_c = tp // 2, lax.rem(tp, 2)
    nbr = {"tp": (1 - me_x) * 2 + me_c}
    partner = {"tp": me_x * 2 + (1 - me_c)}

    def w_copy(t, slot):
        j, k = t // nk, lax.rem(t, nk)
        return pltpu.make_async_copy(
            w_hbm.at[pl.ds(pl.multiple_of(k * KB, KB), KB), pl.ds(pl.multiple_of(j * CN, CN), CN)],
            w_buf.at[slot], w_sem.at[slot])

    def x_copy(k):
        cols = pl.ds(k * KB, KB)
        return pltpu.make_async_copy(x_hbm.at[:, cols], x_buf.at[:, cols], x_sem.at[k])

    for k in range(nk):
        x_copy(k).start()
    for t in range(SLOTS):
        w_copy(t, t).start()

    barrier = pltpu.get_barrier_semaphore()
    for dev in (partner, nbr):
        pl.semaphore_signal(barrier, inc=1, device_id=dev, device_id_type=MESH)

    pos = lax.broadcasted_iota(jnp.int32, (rows, tokens), 0)
    pick = (pos == row_targets(len_ref, (rows, tokens), 1, seq_len)).astype(jnp.bfloat16)
    for k in range(nk):
        x_copy(k).wait()

        @pl.loop(0, KB // 512)
        def _(i):
            cols = pl.ds(pl.multiple_of(k * KB + i * 512, 512), 512)
            xc[:, cols] = jnp.dot(pick, x_buf[:, cols], preferred_element_type=jnp.float32).astype(jnp.bfloat16)

    pl.semaphore_wait(barrier, 2)

    def remote(src, dst, s, r, dev):
        return pltpu.make_async_remote_copy(src_ref=src, dst_ref=dst, send_sem=s, recv_sem=r,
                                            device_id=dev, device_id_type=MESH)

    def d2d_copy(j):
        return remote(part.at[j, 1 - me_c], d2d_in.at[j], d2d_s.at[j], d2d_r.at[j], partner)

    def ici_copy(j):
        return remote(d2d_in.at[j, 1 - me_x], ici_in.at[j], ici_s.at[j], ici_r.at[j], nbr)

    def yx_copy(j):
        q = y_ref.at[j, me_c, me_x]
        return remote(q, q, yx_s.at[j], yx_r.at[j], nbr)

    def yp_copy(j):
        q = y_ref.at[j, me_c, me_x]
        return remote(q, q, yp_s.at[j], yp_r.at[j], partner)

    def yf_copy(j):
        q = y_ref.at[j, me_c, 1 - me_x]
        return remote(q, q, yf_s.at[j], yf_r.at[j], partner)

    def stage_a(j):
        d2d_copy(j).start()

    def stage_b(j):
        d2d_copy(j).wait_recv()
        d2d_in[j, 1 - me_x] = d2d_in[j, 1 - me_x] + part[j, me_c, 1 - me_x]
        d2d_in[j, me_x] = d2d_in[j, me_x] + part[j, me_c, me_x]
        ici_copy(j).start()

    def stage_c(j):
        ici_copy(j).wait_recv()
        y_ref[j, me_c, me_x] = (d2d_in[j, me_x] + ici_in[j]).astype(jnp.bfloat16)
        yx_copy(j).start()
        yp_copy(j).start()

    def stage_d(j):
        yx_copy(j).wait_recv()
        yf_copy(j).start()

    stages = ((stage_b, LAG_B), (stage_c, LAG_C), (stage_d, LAG_D))

    @pl.loop(0, nc)
    def _(j):
        for k in range(nk):
            t = j * nk + k
            slot = lax.rem(t, SLOTS)
            w_copy(t, slot).wait()
            got = jnp.dot(xc[:, k * KB:(k + 1) * KB], w_buf[slot], preferred_element_type=jnp.float32)
            for q in range(4):
                piece = got[:, q * 128:(q + 1) * 128]
                if k:
                    part[j, q // 2, q % 2] += piece
                else:
                    part[j, q // 2, q % 2] = piece

            @pl.when(t + SLOTS < total)
            def _():
                w_copy(t + SLOTS, slot).start()

            if 0 < k <= len(stages):
                stage, lag = stages[k - 1]

                @pl.when(j >= lag)
                def _():
                    stage(j - lag)
        stage_a(j)

    for step in range(nc, nc + LAG_D):
        for stage, lag in stages:
            if step - lag < nc:
                stage(step - lag)

    @pl.loop(0, nc)
    def _(j):
        yp_copy(j).wait_recv()
        yf_copy(j).wait_recv()
        d2d_copy(j).wait_send()
        ici_copy(j).wait_send()
        yx_copy(j).wait_send()
        yp_copy(j).wait_send()
        yf_copy(j).wait_send()


def expand_kernel(len_ref, y_ref, out_ref):
    tokens = out_ref.shape[0]
    rows = y_ref.shape[3]
    seq_len = tokens // len_ref.shape[0]
    pos = lax.broadcasted_iota(jnp.int32, (tokens, rows), 1)
    place = (pos == row_targets(len_ref, (tokens, rows), 0, seq_len)).astype(jnp.bfloat16)
    for i in range(y_ref.shape[0]):
        for q in range(4):
            c = (i * 4 + q) * 128
            out_ref[:, c:c + 128] = jnp.dot(place, y_ref[i, q // 2, q % 2], preferred_element_type=jnp.float32).astype(jnp.bfloat16)


def solution(mesh):
    def local_part(x_loc, w_loc, lengths):
        tokens, depth = x_loc.shape
        width = w_loc.shape[1]
        rows, nc, nk = ROWS, width // CN, depth // KB
        dma = lambda n: pltpu.SemaphoreType.DMA((n,))
        y = pl.pallas_call(
            matmul_kernel,
            out_shape=jax.ShapeDtypeStruct((nc, 2, 2, rows, 128), jnp.bfloat16),
            in_specs=[pl.BlockSpec(memory_space=pltpu.SMEM), pl.BlockSpec(memory_space=pl.ANY), pl.BlockSpec(memory_space=pl.ANY)],
            out_specs=pl.BlockSpec(memory_space=pltpu.VMEM),
            scratch_shapes=[
                pltpu.VMEM((tokens, depth), jnp.bfloat16),
                pltpu.VMEM((rows, depth), jnp.bfloat16),
                pltpu.VMEM((SLOTS, KB, CN), jnp.bfloat16),
                pltpu.VMEM((nc, 2, 2, rows, 128), jnp.float32),
                pltpu.VMEM((nc, 2, rows, 128), jnp.float32),
                pltpu.VMEM((nc, rows, 128), jnp.float32),
                dma(nk), dma(SLOTS)] + [dma(nc)] * 10,
            compiler_params=pltpu.CompilerParams(collective_id=0, has_side_effects=True, vmem_limit_bytes=56 * 2**20),
            cost_estimate=pl.CostEstimate(flops=2 * rows * depth * width, bytes_accessed=2 * depth * width, transcendentals=0),
        )(lengths, x_loc, w_loc)
        step = 2
        return pl.pallas_call(
            expand_kernel,
            out_shape=jax.ShapeDtypeStruct((tokens, width), jnp.bfloat16),
            grid=(nc // step,),
            in_specs=[pl.BlockSpec(memory_space=pltpu.SMEM), pl.BlockSpec((step, 2, 2, rows, 128), lambda i: (i, 0, 0, 0, 0))],
            out_specs=pl.BlockSpec((tokens, step * CN), lambda i: (0, i)),
            cost_estimate=pl.CostEstimate(flops=2 * rows * tokens * width, bytes_accessed=4 * tokens * width, transcendentals=0),
        )(lengths, y)

    return jax.shard_map(local_part, mesh=mesh, in_specs=(P("data", "tp"), P("tp", None), P("data")), out_specs=P("data", None), check_vma=False)
```

```python
import functools

import jax
import jax.numpy as jnp
from jax import lax
from jax.experimental import pallas as pl
from jax.experimental.pallas import tpu as pltpu
from jax.sharding import PartitionSpec as P

MESH = pl.DeviceIdType.MESH
CAPS = (128, 144, 160, 176, 192, 208)
CN = 512
KB = 4096
SLOTS = 6
FIRST = 1
LAG_B, LAG_C, LAG_D = 1, 3, 5
RING = 8


def row_targets(len_ref, shape, axis, seq_len):
    row = lax.broadcasted_iota(jnp.int32, shape, axis)
    target = jnp.full(shape, -1, jnp.int32)
    start = jnp.int32(0)
    for s in range(len_ref.shape[0]):
        inside = (row >= s * seq_len) & (row < s * seq_len + len_ref[s])
        target = jnp.where(inside, row - s * seq_len + start, target)
        start = start + len_ref[s]
    return target


def head_kernel(len_ref, x_hbm, w_hbm, pick_ref, xc_out, part_out, x_buf, xc, w_buf, part, mine, theirs,
                x_sem, w_sem, o_sem, p_sem, send, recv):
    tokens, depth = x_hbm.shape
    rows = xc.shape[0]
    nk = depth // KB
    seq_len = tokens // len_ref.shape[0]
    groups = theirs.shape[0] + 1
    me = lax.axis_index("data")
    peers = [{"data": lax.rem(me + r, groups)} for r in range(1, groups)]

    def x_copy(k):
        cols = pl.ds(k * KB, KB)
        return pltpu.make_async_copy(x_hbm.at[:, cols], x_buf.at[:, cols], x_sem.at[k])

    def w_copy(t):
        j, k = t // nk, t % nk
        return pltpu.make_async_copy(w_hbm.at[pl.ds(k * KB, KB), pl.ds(j * CN, CN)], w_buf.at[t], w_sem.at[t])

    def xc_copy(k):
        cols = pl.ds(k * KB, KB)
        return pltpu.make_async_copy(xc.at[:, cols], xc_out.at[:, cols], o_sem.at[k])

    def tell(r):
        return pltpu.make_async_remote_copy(src_ref=mine, dst_ref=theirs.at[r], send_sem=send.at[r], recv_sem=recv.at[r],
                                            device_id=peers[r], device_id_type=MESH)

    for k in range(nk):
        x_copy(k).start()
    for t in range(FIRST * nk):
        w_copy(t).start()
    barrier = pltpu.get_barrier_semaphore()
    for dev in peers:
        pl.semaphore_signal(barrier, inc=1, device_id=dev, device_id_type=MESH)
    total = len_ref[0]
    for s in range(1, len_ref.shape[0]):
        total = total + len_ref[s]
    mine[...] = jnp.full(mine.shape, total, jnp.int32)

    pos = lax.broadcasted_iota(jnp.int32, (rows, tokens), 0)
    pick = (pos == row_targets(len_ref, (rows, tokens), 1, seq_len)).astype(jnp.bfloat16)
    pl.semaphore_wait(barrier, groups - 1)
    for r in range(groups - 1):
        tell(r).start()
    for k in range(nk):
        x_copy(k).wait()

        @pl.loop(0, KB // 1024)
        def _(i):
            cols = pl.ds(pl.multiple_of(k * KB + i * 1024, 1024), 1024)
            xc[:, cols] = jnp.dot(pick, x_buf[:, cols], preferred_element_type=jnp.float32).astype(jnp.bfloat16)

    for t in range(FIRST * nk):
        j, k = t // nk, t % nk
        w_copy(t).wait()
        got = jnp.dot(xc[:, k * KB:(k + 1) * KB], w_buf[t], preferred_element_type=jnp.float32)
        for q in range(4):
            piece = got[:, q * 128:(q + 1) * 128]
            part[j, q // 2, q % 2] = part[j, q // 2, q % 2] + piece if k else piece
        if t == 0:
            for i in range(nk):
                xc_copy(i).start()

    p_copy = pltpu.make_async_copy(part, part_out, p_sem)
    p_copy.start()
    most = mine[...]
    for r in range(groups - 1):
        tell(r).wait()
        most = jnp.maximum(most, theirs[r])
    most = jnp.max(most)
    index = jnp.int32(0)
    for cap in CAPS[:-1]:
        index = index + (most > cap).astype(jnp.int32)
    pick_ref[0] = index
    for k in range(nk):
        xc_copy(k).wait()
    p_copy.wait()


def main_kernel(xc_hbm, part_hbm, w_hbm, y_out, xc, w_buf, part, d2d_in, ici_in, own, other,
                x_sem, p_sem, w_sem, d2d_s, d2d_r, ici_s, ici_r, yx_s, yx_r, yp_s, yp_r, yf_s, yf_r, yl_s, yo_s):
    rows, depth = xc.shape
    width = w_hbm.shape[1]
    nc, nk = width // CN, depth // KB
    total = nc * nk
    tp = lax.axis_index("tp")
    me_x, me_c = tp // 2, lax.rem(tp, 2)
    nbr = {"tp": (1 - me_x) * 2 + me_c}
    partner = {"tp": me_x * 2 + (1 - me_c)}

    def w_copy(t, slot):
        j, k = t // nk, lax.rem(t, nk)
        return pltpu.make_async_copy(
            w_hbm.at[pl.ds(pl.multiple_of(k * KB, KB), KB), pl.ds(pl.multiple_of(j * CN, CN), CN)],
            w_buf.at[slot], w_sem.at[slot])

    def x_copy(k):
        cols = pl.ds(k * KB, KB)
        return pltpu.make_async_copy(xc_hbm.at[pl.ds(0, rows), cols], xc.at[:, cols], x_sem.at[k])

    p_copy = pltpu.make_async_copy(part_hbm.at[:, :, :, pl.ds(0, rows)], part.at[pl.ds(0, FIRST)], p_sem)

    barrier = pltpu.get_barrier_semaphore()
    for dev in (partner, nbr):
        pl.semaphore_signal(barrier, inc=1, device_id=dev, device_id_type=MESH)
    p_copy.start()
    for k in range(nk):
        x_copy(k).start()
    for t in range(FIRST * nk, FIRST * nk + SLOTS):
        w_copy(t, t % SLOTS).start()

    def remote(src, dst, s, r, dev):
        return pltpu.make_async_remote_copy(src_ref=src, dst_ref=dst, send_sem=s, recv_sem=r,
                                            device_id=dev, device_id_type=MESH)

    def d2d_copy(j):
        return remote(part.at[j, 1 - me_c], d2d_in.at[j], d2d_s, d2d_r.at[lax.rem(j, 4)], partner)

    def ici_copy(j):
        return remote(d2d_in.at[j, 1 - me_x], ici_in.at[j], ici_s, ici_r.at[lax.rem(j, RING)], nbr)

    def yx_copy(j):
        return remote(own.at[j], other.at[j], yx_s, yx_r.at[lax.rem(j, RING)], nbr)

    def yp_copy(j):
        return remote(own.at[j], y_out.at[j, me_c, me_x], yp_s, yp_r, partner)

    def yf_copy(j):
        return remote(other.at[j], y_out.at[j, me_c, 1 - me_x], yf_s, yf_r, partner)

    def yl_copy(j):
        return pltpu.make_async_copy(own.at[j], y_out.at[j, me_c, me_x], yl_s)

    def yo_copy(j):
        return pltpu.make_async_copy(other.at[j], y_out.at[j, me_c, 1 - me_x], yo_s)

    def stage_a(j):
        d2d_copy(j).start()

    def stage_b(j):
        d2d_copy(j).wait_recv()
        d2d_in[j, 1 - me_x] = d2d_in[j, 1 - me_x] + part[j, me_c, 1 - me_x]
        d2d_in[j, me_x] = d2d_in[j, me_x] + part[j, me_c, me_x]
        ici_copy(j).start()

    def stage_c(j):
        ici_copy(j).wait_recv()
        own[j] = (d2d_in[j, me_x] + ici_in[j]).astype(jnp.bfloat16)
        yx_copy(j).start()
        yp_copy(j).start()
        yl_copy(j).start()

    def stage_d(j):
        yx_copy(j).wait_recv()
        yf_copy(j).start()
        yo_copy(j).start()

    def when_late(j, lag, stage):
        @pl.when(j >= lag)
        def _():
            stage(j - lag)

    p_copy.wait()
    pl.semaphore_wait(barrier, 2)
    for j in range(FIRST):
        stage_a(j)
    for k in range(nk):
        x_copy(k).wait()

    @pl.loop(FIRST, nc)
    def _(j):
        for k in range(nk):
            t = j * nk + k
            slot = lax.rem(t, SLOTS)
            w_copy(t, slot).wait()
            got = jnp.dot(xc[:, k * KB:(k + 1) * KB], w_buf[slot], preferred_element_type=jnp.float32)
            for q in range(4):
                piece = got[:, q * 128:(q + 1) * 128]
                if k:
                    part[j, q // 2, q % 2] += piece
                else:
                    part[j, q // 2, q % 2] = piece

            @pl.when(t + SLOTS < total)
            def _():
                w_copy(t + SLOTS, slot).start()

            if k == 0:
                when_late(j, LAG_B, stage_b)
                when_late(j, LAG_C, stage_c)
        when_late(j, LAG_D, stage_d)
        stage_a(j)

    for step in range(nc, nc + LAG_D):
        for stage, lag in ((stage_b, LAG_B), (stage_c, LAG_C), (stage_d, LAG_D)):
            if step - lag < nc:
                stage(step - lag)

    for buf, sems in ((own, (yp_r, yf_r, yl_s, yo_s, yx_s, yp_s, yf_s)), (d2d_in, (d2d_s,)), (ici_in, (ici_s,))):
        for sem in sems:
            pltpu.make_async_copy(buf, buf, sem).wait()


def expand_kernel(len_ref, y_ref, out_hbm, buf, sem):
    tokens = out_hbm.shape[0]
    rows = y_ref.shape[3]
    seq_len = tokens // len_ref.shape[0]
    pos = lax.broadcasted_iota(jnp.int32, (tokens, rows), 1)
    place = (pos == row_targets(len_ref, (tokens, rows), 0, seq_len)).astype(jnp.bfloat16)
    steps, _, cols = buf.shape
    chunks = cols // CN

    def out_copy(i):
        return pltpu.make_async_copy(buf.at[i], out_hbm.at[:, pl.ds(i * cols, cols)], sem.at[i])

    for i in range(steps):
        wide = jnp.concatenate([y_ref[i * chunks + u, q // 2, q % 2] for u in range(chunks) for q in range(4)], axis=1)
        buf[i] = jnp.dot(place, wide, preferred_element_type=jnp.float32).astype(jnp.bfloat16)
        out_copy(i).start()
    for i in range(steps):
        out_copy(i).wait()


def solution(mesh):
    smem, hbm, vmem, anywhere = (pl.BlockSpec(memory_space=m) for m in (pltpu.SMEM, pltpu.HBM, pltpu.VMEM, pl.ANY))
    dma = lambda n: pltpu.SemaphoreType.DMA((n,))
    one = pltpu.SemaphoreType.DMA
    most = CAPS[-1]

    def with_rows(rows, xc, part, w_loc, lengths):
        depth, width = w_loc.shape
        tokens = 256
        nc, nk = width // CN, depth // KB
        y = pl.pallas_call(
            main_kernel,
            out_shape=jax.ShapeDtypeStruct((nc, 2, 2, rows, 128), jnp.bfloat16),
            in_specs=[anywhere, anywhere, hbm],
            out_specs=anywhere,
            scratch_shapes=[
                pltpu.VMEM((rows, depth), jnp.bfloat16),
                pltpu.VMEM((SLOTS, KB, CN), jnp.bfloat16),
                pltpu.VMEM((nc, 2, 2, rows, 128), jnp.float32),
                pltpu.VMEM((nc, 2, rows, 128), jnp.float32),
                pltpu.VMEM((nc, rows, 128), jnp.float32),
                pltpu.VMEM((nc, rows, 128), jnp.bfloat16),
                pltpu.VMEM((nc, rows, 128), jnp.bfloat16),
                dma(nk), one, dma(SLOTS), one, dma(4), one, dma(RING), one, dma(RING), one, one, one, one, one, one],
            compiler_params=pltpu.CompilerParams(collective_id=1 + CAPS.index(rows), has_side_effects=True, vmem_limit_bytes=44 * 2**20),
            cost_estimate=pl.CostEstimate(flops=2 * rows * depth * width, bytes_accessed=2 * depth * width, transcendentals=0),
        )(xc, part, w_loc)
        steps = nc // 2
        return pl.pallas_call(
            expand_kernel,
            out_shape=pltpu.HBM((tokens, width), jnp.bfloat16),
            in_specs=[smem, vmem],
            out_specs=hbm,
            scratch_shapes=[pltpu.VMEM((steps, tokens, width // steps), jnp.bfloat16), dma(steps)],
            compiler_params=pltpu.CompilerParams(vmem_limit_bytes=16 * 2**20),
            cost_estimate=pl.CostEstimate(flops=2 * rows * tokens * width, bytes_accessed=4 * tokens * width, transcendentals=0),
        )(lengths, y)

    def local_part(x_loc, w_loc, lengths):
        tokens, depth = x_loc.shape
        nk = depth // KB
        groups = mesh.shape["data"]
        pick, xc, part = pl.pallas_call(
            head_kernel,
            out_shape=[jax.ShapeDtypeStruct((1,), jnp.int32), jax.ShapeDtypeStruct((most, depth), jnp.bfloat16),
                       jax.ShapeDtypeStruct((FIRST, 2, 2, most, 128), jnp.float32)],
            in_specs=[smem, hbm, hbm],
            out_specs=[smem, anywhere, anywhere],
            scratch_shapes=[
                pltpu.VMEM((tokens, depth), jnp.bfloat16),
                pltpu.VMEM((most, depth), jnp.bfloat16),
                pltpu.VMEM((FIRST * nk, KB, CN), jnp.bfloat16),
                pltpu.VMEM((FIRST, 2, 2, most, 128), jnp.float32),
                pltpu.VMEM((8, 128), jnp.int32),
                pltpu.VMEM((groups - 1, 8, 128), jnp.int32),
                dma(nk), dma(FIRST * nk), dma(nk), one, dma(groups - 1), dma(groups - 1)],
            compiler_params=pltpu.CompilerParams(collective_id=0, has_side_effects=True, vmem_limit_bytes=60 * 2**20),
            cost_estimate=pl.CostEstimate(flops=2 * most * depth * CN, bytes_accessed=2 * depth * CN, transcendentals=0),
        )(lengths, x_loc, w_loc)
        return lax.switch(pick[0], [functools.partial(with_rows, cap) for cap in CAPS], xc, part, w_loc, lengths)

    return jax.shard_map(local_part, mesh=mesh, in_specs=(P("data", "tp"), P("tp", None), P("data")), out_specs=P("data", None), check_vma=False)
```

```python
import functools

import jax
import jax.numpy as jnp
from jax import lax
from jax.experimental import pallas as pl
from jax.experimental.pallas import tpu as pltpu
from jax.sharding import PartitionSpec as P

MESH = pl.DeviceIdType.MESH
CAPS = (120, 128, 136, 144, 152, 160, 168, 176, 184, 200)
CN = 512
KB = 4096
XB = 2048
SLOTS = 6
FIRST = 1
LAG_B, LAG_C, LAG_D = 1, 3, 5
RING = 8


def row_targets(len_ref, shape, axis, seq_len):
    row = lax.broadcasted_iota(jnp.int32, shape, axis)
    target = jnp.full(shape, -1, jnp.int32)
    start = jnp.int32(0)
    for s in range(len_ref.shape[0]):
        inside = (row >= s * seq_len) & (row < s * seq_len + len_ref[s])
        target = jnp.where(inside, row - s * seq_len + start, target)
        start = start + len_ref[s]
    return target


def head_kernel(len_ref, x_hbm, w_hbm, pick_ref, xc, *rest):
    if FIRST:
        part, x_buf, mine, theirs, x_sem, send, recv, w_buf, w_sem = rest
    else:
        x_buf, mine, theirs, x_sem, send, recv = rest
    tokens, depth = x_hbm.shape
    rows = xc.shape[0]
    nk, nx = depth // KB, depth // XB
    seq_len = tokens // len_ref.shape[0]
    groups = theirs.shape[0] + 1
    me = lax.axis_index("data")
    peers = [{"data": lax.rem(me + r, groups)} for r in range(1, groups)]

    def x_copy(k):
        cols = pl.ds(pl.multiple_of(k * XB, XB), XB)
        return pltpu.make_async_copy(x_hbm.at[:, cols], x_buf.at[:, cols], x_sem.at[k])

    def w_copy(t):
        j, k = t // nk, t % nk
        return pltpu.make_async_copy(w_hbm.at[pl.ds(pl.multiple_of(k * KB, KB), KB), pl.ds(pl.multiple_of(j * CN, CN), CN)], w_buf.at[t], w_sem.at[t])

    def tell(r):
        return pltpu.make_async_remote_copy(src_ref=mine, dst_ref=theirs.at[r], send_sem=send.at[r], recv_sem=recv.at[r],
                                            device_id=peers[r], device_id_type=MESH)

    barrier = pltpu.get_barrier_semaphore()
    for dev in peers:
        pl.semaphore_signal(barrier, inc=1, device_id=dev, device_id_type=MESH)
    for k in range(nx):
        x_copy(k).start()
    for t in range(FIRST * nk):
        w_copy(t).start()
    total = len_ref[0]
    for s in range(1, len_ref.shape[0]):
        total = total + len_ref[s]
    mine[...] = jnp.full(mine.shape, total, jnp.int32)

    pos = lax.broadcasted_iota(jnp.int32, (rows, tokens), 0)
    pick = (pos == row_targets(len_ref, (rows, tokens), 1, seq_len)).astype(jnp.bfloat16)
    pl.semaphore_wait(barrier, groups - 1)
    for r in range(groups - 1):
        tell(r).start()

    @pl.loop(0, nx)
    def _(k):
        x_copy(k).wait()
        cols = pl.ds(pl.multiple_of(k * XB, XB), XB)
        xc[:, cols] = jnp.dot(pick, x_buf[:, cols], preferred_element_type=jnp.float32).astype(jnp.bfloat16)

    @pl.loop(0, FIRST * nk)
    def _(t):
        j, k = t // nk, lax.rem(t, nk)
        w_copy(t).wait()
        got = jnp.dot(xc[:, pl.ds(pl.multiple_of(k * KB, KB), KB)], w_buf[t], preferred_element_type=jnp.float32)
        for q in range(4):
            before = jnp.where(k == 0, 0.0, part[j, q // 2, q % 2])
            part[j, q // 2, q % 2] = before + got[:, q * 128:(q + 1) * 128]

    most = mine[...]
    for r in range(groups - 1):
        tell(r).wait()
        most = jnp.maximum(most, theirs[r])
    most = jnp.max(most)
    index = jnp.int32(0)
    for cap in CAPS[:-1]:
        index = index + (most > cap).astype(jnp.int32)
    pick_ref[0] = index


def main_kernel(*refs):
    xc, *first, w_hbm, y_out = refs[:3 + bool(FIRST)]
    (w_buf, part, d2d_in, ici_in, own, other, w_sem, d2d_s, d2d_r, ici_s, ici_r, yx_s, yx_r, yp_s, yp_r, yf_s, yf_r, yl_s, yo_s) = refs[3 + bool(FIRST):]
    rows, depth = part.shape[3], xc.shape[1]
    width = w_hbm.shape[1]
    nc, nk = width // CN, depth // KB
    total = nc * nk
    tp = lax.axis_index("tp")
    me_x, me_c = tp // 2, lax.rem(tp, 2)
    nbr = {"tp": (1 - me_x) * 2 + me_c}
    partner = {"tp": me_x * 2 + (1 - me_c)}

    def w_copy(t, slot):
        j, k = t // nk, lax.rem(t, nk)
        return pltpu.make_async_copy(
            w_hbm.at[pl.ds(pl.multiple_of(k * KB, KB), KB), pl.ds(pl.multiple_of(j * CN, CN), CN)],
            w_buf.at[slot], w_sem.at[slot])

    barrier = pltpu.get_barrier_semaphore()
    for dev in (partner, nbr):
        pl.semaphore_signal(barrier, inc=1, device_id=dev, device_id_type=MESH)
    for t in range(FIRST * nk, FIRST * nk + SLOTS):
        w_copy(t, t % SLOTS).start()

    def remote(src, dst, s, r, dev):
        return pltpu.make_async_remote_copy(src_ref=src, dst_ref=dst, send_sem=s, recv_sem=r,
                                            device_id=dev, device_id_type=MESH)

    def d2d_copy(j):
        return remote(part.at[j, 1 - me_c], d2d_in.at[j], d2d_s, d2d_r.at[lax.rem(j, 4)], partner)

    def ici_copy(j):
        return remote(d2d_in.at[j, 1 - me_x], ici_in.at[j], ici_s, ici_r.at[lax.rem(j, RING)], nbr)

    def yx_copy(j):
        return remote(own.at[j], other.at[j], yx_s, yx_r.at[lax.rem(j, RING)], nbr)

    def yp_copy(j):
        return remote(own.at[j], y_out.at[j, me_c, me_x], yp_s, yp_r, partner)

    def yf_copy(j):
        return remote(other.at[j], y_out.at[j, me_c, 1 - me_x], yf_s, yf_r, partner)

    def yl_copy(j):
        return pltpu.make_async_copy(own.at[j], y_out.at[j, me_c, me_x], yl_s)

    def yo_copy(j):
        return pltpu.make_async_copy(other.at[j], y_out.at[j, me_c, 1 - me_x], yo_s)

    def stage_a(j):
        d2d_copy(j).start()

    def stage_b(j):
        d2d_copy(j).wait_recv()
        d2d_in[j, 1 - me_x] = d2d_in[j, 1 - me_x] + part[j, me_c, 1 - me_x]
        d2d_in[j, me_x] = d2d_in[j, me_x] + part[j, me_c, me_x]
        ici_copy(j).start()

    def stage_c(j):
        ici_copy(j).wait_recv()
        own[j] = (d2d_in[j, me_x] + ici_in[j]).astype(jnp.bfloat16)
        yx_copy(j).start()
        yp_copy(j).start()
        yl_copy(j).start()

    def stage_d(j):
        yx_copy(j).wait_recv()
        yf_copy(j).start()
        yo_copy(j).start()

    def when_valid(j, stage, least=0):
        @pl.when((j >= least) & (j < nc))
        def _():
            stage(j)

    for j in range(FIRST):
        for q in range(4):
            part[j, q // 2, q % 2] = first[0][j, q // 2, q % 2, :rows]
    pl.semaphore_wait(barrier, 2)
    for j in range(FIRST):
        stage_a(j)
        stage_b(j)

    @pl.loop(FIRST * nk, (nc + LAG_D) * nk)
    def _(t):
        j, k = t // nk, lax.rem(t, nk)

        @pl.when(t < total)
        def _():
            slot = lax.rem(t, SLOTS)
            w_copy(t, slot).wait()
            got = jnp.dot(xc[:rows, pl.ds(pl.multiple_of(k * KB, KB), KB)], w_buf[slot], preferred_element_type=jnp.float32)
            for q in range(4):
                before = jnp.where(k == 0, 0.0, part[j, q // 2, q % 2])
                part[j, q // 2, q % 2] = before + got[:, q * 128:(q + 1) * 128]

            @pl.when(t + SLOTS < total)
            def _():
                w_copy(t + SLOTS, slot).start()

        @pl.when(k == 0)
        def _():
            when_valid(j - LAG_B, stage_b, FIRST)
            when_valid(j - LAG_C, stage_c)

        @pl.when(k == nk - 1)
        def _():
            when_valid(j, stage_a)
            when_valid(j - LAG_D, stage_d)

    for buf, sems in ((own, (yp_r, yf_r, yl_s, yo_s, yx_s, yp_s, yf_s)), (d2d_in, (d2d_s,)), (ici_in, (ici_s,))):
        for sem in sems:
            pltpu.make_async_copy(buf, buf, sem).wait()


def expand_kernel(len_ref, y_ref, out_hbm, buf, sem):
    tokens = out_hbm.shape[0]
    rows = y_ref.shape[3]
    seq_len = tokens // len_ref.shape[0]
    pos = lax.broadcasted_iota(jnp.int32, (tokens, rows), 1)
    place = (pos == row_targets(len_ref, (tokens, rows), 0, seq_len)).astype(jnp.bfloat16)
    steps, _, cols = buf.shape
    chunks = cols // CN

    def out_copy(i):
        return pltpu.make_async_copy(buf.at[i], out_hbm.at[:, pl.ds(i * cols, cols)], sem.at[i])

    for i in range(steps):
        wide = jnp.concatenate([y_ref[i * chunks + u, q // 2, q % 2] for u in range(chunks) for q in range(4)], axis=1)
        buf[i] = jnp.dot(place, wide, preferred_element_type=jnp.float32).astype(jnp.bfloat16)
        out_copy(i).start()
    for i in range(steps):
        out_copy(i).wait()


def solution(mesh):
    smem, hbm, vmem, anywhere = (pl.BlockSpec(memory_space=m) for m in (pltpu.SMEM, pltpu.HBM, pltpu.VMEM, pl.ANY))
    dma = lambda n: pltpu.SemaphoreType.DMA((n,))
    one = pltpu.SemaphoreType.DMA
    most = 208

    def with_rows(rows, have, w_loc, lengths):
        depth, width = w_loc.shape
        tokens = 256
        nc, nk = width // CN, depth // KB
        y = pl.pallas_call(
            main_kernel,
            out_shape=jax.ShapeDtypeStruct((nc, 2, 2, rows, 128), jnp.bfloat16),
            in_specs=[vmem] * len(have) + [hbm],
            out_specs=anywhere,
            scratch_shapes=[
                pltpu.VMEM((SLOTS, KB, CN), jnp.bfloat16),
                pltpu.VMEM((nc, 2, 2, rows, 128), jnp.float32),
                pltpu.VMEM((nc, 2, rows, 128), jnp.float32),
                pltpu.VMEM((nc, rows, 128), jnp.float32),
                pltpu.VMEM((nc, rows, 128), jnp.bfloat16),
                pltpu.VMEM((nc, rows, 128), jnp.bfloat16),
                dma(SLOTS), one, dma(4), one, dma(RING), one, dma(RING), one, one, one, one, one, one],
            compiler_params=pltpu.CompilerParams(collective_id=1 + CAPS.index(rows), has_side_effects=True, vmem_limit_bytes=44 * 2**20),
            cost_estimate=pl.CostEstimate(flops=2 * rows * depth * width, bytes_accessed=2 * depth * width, transcendentals=0),
        )(*have, w_loc)
        steps = nc // 2
        return pl.pallas_call(
            expand_kernel,
            out_shape=pltpu.HBM((tokens, width), jnp.bfloat16),
            in_specs=[smem, vmem],
            out_specs=hbm,
            scratch_shapes=[pltpu.VMEM((steps, tokens, width // steps), jnp.bfloat16), dma(steps)],
            compiler_params=pltpu.CompilerParams(vmem_limit_bytes=16 * 2**20),
            cost_estimate=pl.CostEstimate(flops=2 * rows * tokens * width, bytes_accessed=4 * tokens * width, transcendentals=0),
        )(lengths, y)

    def local_part(x_loc, w_loc, lengths):
        tokens, depth = x_loc.shape
        nk = depth // KB
        groups = mesh.shape["data"]
        out_shape = [jax.ShapeDtypeStruct((1,), jnp.int32), pltpu.VMEM((most, depth), jnp.bfloat16)]
        scratch = [pltpu.VMEM((tokens, depth), jnp.bfloat16), pltpu.VMEM((8, 128), jnp.int32), pltpu.VMEM((groups - 1, 8, 128), jnp.int32),
                   dma(depth // XB), dma(groups - 1), dma(groups - 1)]
        if FIRST:
            out_shape.append(pltpu.VMEM((FIRST, 2, 2, most, 128), jnp.float32))
            scratch += [pltpu.VMEM((FIRST * nk, KB, CN), jnp.bfloat16), dma(FIRST * nk)]
        pick, *have = pl.pallas_call(
            head_kernel,
            out_shape=out_shape,
            in_specs=[smem, hbm, hbm],
            out_specs=[smem] + [vmem] * (len(out_shape) - 1),
            scratch_shapes=scratch,
            compiler_params=pltpu.CompilerParams(collective_id=0, has_side_effects=True, vmem_limit_bytes=(12 + FIRST * 12) * 2**20),
            cost_estimate=pl.CostEstimate(flops=2 * most * depth * CN, bytes_accessed=2 * depth * CN, transcendentals=0),
        )(lengths, pltpu.with_memory_space_constraint(x_loc, pltpu.HBM), w_loc)
        return lax.switch(pick[0], [functools.partial(with_rows, cap) for cap in CAPS], have, w_loc, lengths)

    return jax.shard_map(local_part, mesh=mesh, in_specs=(P("data", "tp"), P("tp", None), P("data")), out_specs=P("data", None), check_vma=False)
```

```python
import functools

import jax
import jax.numpy as jnp
from jax import lax
from jax.experimental import pallas as pl
from jax.experimental.pallas import tpu as pltpu
from jax.sharding import PartitionSpec as P

MESH = pl.DeviceIdType.MESH
CAPS = (120, 128, 136, 144, 152, 160, 168, 176, 184, 200)
CN = 512
KB = 4096
XB = 4096
SLOTS = 6
FIRST = 1
AHEAD = 1
LAG_B, LAG_C, LAG_D = 1, 3, 5
RING = 8


def row_targets(len_ref, shape, axis, seq_len):
    row = lax.broadcasted_iota(jnp.int32, shape, axis)
    target = jnp.full(shape, -1, jnp.int32)
    start = jnp.int32(0)
    for s in range(len_ref.shape[0]):
        inside = (row >= s * seq_len) & (row < s * seq_len + len_ref[s])
        target = jnp.where(inside, row - s * seq_len + start, target)
        start = start + len_ref[s]
    return target


def head_kernel(len_ref, x_hbm, w_hbm, pick_ref, xc, *rest):
    part, ahead, x_buf, mine, theirs, x_sem, send, recv, w_buf, w_sem, a_sem = rest
    tokens, depth = x_hbm.shape
    rows = xc.shape[0]
    nk, nx = depth // KB, depth // XB
    seq_len = tokens // len_ref.shape[0]
    groups = theirs.shape[0] + 1
    me = lax.axis_index("data")
    peers = [{"data": lax.rem(me + r, groups)} for r in range(1, groups)]

    def x_copy(k):
        cols = pl.ds(pl.multiple_of(k * XB, XB), XB)
        return pltpu.make_async_copy(x_hbm.at[:, cols], x_buf.at[:, cols], x_sem.at[k])

    def w_copy(t):
        j, k = t // nk, t % nk
        return pltpu.make_async_copy(w_hbm.at[pl.ds(pl.multiple_of(k * KB, KB), KB), pl.ds(pl.multiple_of(j * CN, CN), CN)], w_buf.at[t], w_sem.at[t])

    def a_copy(k):
        return pltpu.make_async_copy(w_hbm.at[pl.ds(k * KB, KB), pl.ds(FIRST * CN, CN)], ahead.at[k], a_sem.at[k])

    def tell(r):
        return pltpu.make_async_remote_copy(src_ref=mine, dst_ref=theirs.at[r], send_sem=send.at[r], recv_sem=recv.at[r],
                                            device_id=peers[r], device_id_type=MESH)

    barrier = pltpu.get_barrier_semaphore()
    for dev in peers:
        pl.semaphore_signal(barrier, inc=1, device_id=dev, device_id_type=MESH)
    for k in range(nx):
        x_copy(k).start()
    for t in range(FIRST * nk):
        w_copy(t).start()
    for k in range(AHEAD):
        a_copy(k).start()
    total = len_ref[0]
    for s in range(1, len_ref.shape[0]):
        total = total + len_ref[s]
    mine[...] = jnp.full(mine.shape, total, jnp.int32)

    pos = lax.broadcasted_iota(jnp.int32, (rows, tokens), 0)
    pick = (pos == row_targets(len_ref, (rows, tokens), 1, seq_len)).astype(jnp.bfloat16)
    pl.semaphore_wait(barrier, groups - 1)
    for r in range(groups - 1):
        tell(r).start()

    @pl.loop(0, nx)
    def _(k):
        x_copy(k).wait()
        cols = pl.ds(pl.multiple_of(k * XB, XB), XB)
        xc[:, cols] = jnp.dot(pick, x_buf[:, cols], preferred_element_type=jnp.float32).astype(jnp.bfloat16)

    @pl.loop(0, FIRST * nk)
    def _(t):
        j, k = t // nk, lax.rem(t, nk)
        w_copy(t).wait()
        got = jnp.dot(xc[:, pl.ds(pl.multiple_of(k * KB, KB), KB)], w_buf[t], preferred_element_type=jnp.float32)
        for q in range(4):
            before = jnp.where(k == 0, 0.0, part[j, q // 2, q % 2])
            part[j, q // 2, q % 2] = before + got[:, q * 128:(q + 1) * 128]

    most = mine[...]
    for r in range(groups - 1):
        tell(r).wait()
        most = jnp.maximum(most, theirs[r])
    most = jnp.max(most)
    index = jnp.int32(0)
    for cap in CAPS[:-1]:
        index = index + (most > cap).astype(jnp.int32)
    pick_ref[0] = index
    for k in range(AHEAD):
        a_copy(k).wait()


def main_kernel(*refs):
    xc, first, ahead, w_hbm, y_out = refs[:5]
    (w_buf, part, d2d_in, ici_in, own, other, w_sem, d2d_s, d2d_r, ici_s, ici_r, yx_s, yx_r, yp_s, yp_r, yf_s, yf_r, yl_s, yo_s) = refs[5:]
    rows, depth = part.shape[3], xc.shape[1]
    width = w_hbm.shape[1]
    nc, nk = width // CN, depth // KB
    total = nc * nk
    tp = lax.axis_index("tp")
    me_x, me_c = tp // 2, lax.rem(tp, 2)
    nbr = {"tp": (1 - me_x) * 2 + me_c}
    partner = {"tp": me_x * 2 + (1 - me_c)}

    def w_copy(t, slot):
        j, k = t // nk, lax.rem(t, nk)
        return pltpu.make_async_copy(
            w_hbm.at[pl.ds(pl.multiple_of(k * KB, KB), KB), pl.ds(pl.multiple_of(j * CN, CN), CN)],
            w_buf.at[slot], w_sem.at[slot])

    barrier = pltpu.get_barrier_semaphore()
    for dev in (partner, nbr):
        pl.semaphore_signal(barrier, inc=1, device_id=dev, device_id_type=MESH)
    begin = FIRST * nk + AHEAD
    for t in range(begin, begin + SLOTS):
        w_copy(t, t % SLOTS).start()

    def remote(src, dst, s, r, dev):
        return pltpu.make_async_remote_copy(src_ref=src, dst_ref=dst, send_sem=s, recv_sem=r,
                                            device_id=dev, device_id_type=MESH)

    def d2d_copy(j):
        return remote(part.at[j, 1 - me_c], d2d_in.at[j], d2d_s, d2d_r.at[lax.rem(j, 4)], partner)

    def ici_copy(j):
        return remote(d2d_in.at[j, 1 - me_x], ici_in.at[j], ici_s, ici_r.at[lax.rem(j, RING)], nbr)

    def yx_copy(j):
        return remote(own.at[j], other.at[j], yx_s, yx_r.at[lax.rem(j, RING)], nbr)

    def yp_copy(j):
        return remote(own.at[j], y_out.at[j, me_c, me_x], yp_s, yp_r, partner)

    def yf_copy(j):
        return remote(other.at[j], y_out.at[j, me_c, 1 - me_x], yf_s, yf_r, partner)

    def yl_copy(j):
        return pltpu.make_async_copy(own.at[j], y_out.at[j, me_c, me_x], yl_s)

    def yo_copy(j):
        return pltpu.make_async_copy(other.at[j], y_out.at[j, me_c, 1 - me_x], yo_s)

    def stage_a(j):
        d2d_copy(j).start()

    def stage_b(j):
        d2d_copy(j).wait_recv()
        d2d_in[j, 1 - me_x] = d2d_in[j, 1 - me_x] + part[j, me_c, 1 - me_x]
        d2d_in[j, me_x] = d2d_in[j, me_x] + part[j, me_c, me_x]
        ici_copy(j).start()

    def stage_c(j):
        ici_copy(j).wait_recv()
        own[j] = (d2d_in[j, me_x] + ici_in[j]).astype(jnp.bfloat16)
        yx_copy(j).start()
        yp_copy(j).start()
        yl_copy(j).start()

    def stage_d(j):
        yx_copy(j).wait_recv()
        yf_copy(j).start()
        yo_copy(j).start()

    def when_valid(j, stage, least=0):
        @pl.when((j >= least) & (j < nc))
        def _():
            stage(j)

    for j in range(FIRST):
        for q in range(4):
            part[j, q // 2, q % 2] = first[j, q // 2, q % 2, :rows]
    pl.semaphore_wait(barrier, 2)
    for j in range(FIRST):
        stage_a(j)
        stage_b(j)

    def multiply(w, j, k):
        got = jnp.dot(xc[:rows, pl.ds(pl.multiple_of(k * KB, KB), KB)], w[...], preferred_element_type=jnp.float32)
        for q in range(4):
            before = jnp.where(k == 0, 0.0, part[j, q // 2, q % 2])
            part[j, q // 2, q % 2] = before + got[:, q * 128:(q + 1) * 128]

    @pl.loop(0, AHEAD)
    def _(k):
        multiply(ahead.at[k], FIRST, k)

    @pl.loop(begin, (nc + LAG_D) * nk)
    def _(t):
        j, k = t // nk, lax.rem(t, nk)

        @pl.when(t < total)
        def _():
            slot = lax.rem(t, SLOTS)
            w_copy(t, slot).wait()
            multiply(w_buf.at[slot], j, k)

            @pl.when(t + SLOTS < total)
            def _():
                w_copy(t + SLOTS, slot).start()

        @pl.when(k == 0)
        def _():
            when_valid(j - LAG_B, stage_b, FIRST)
            when_valid(j - LAG_C, stage_c)

        @pl.when(k == nk - 1)
        def _():
            when_valid(j, stage_a)
            when_valid(j - LAG_D, stage_d)

    for buf, sems in ((own, (yp_r, yf_r, yl_s, yo_s, yx_s, yp_s, yf_s)), (d2d_in, (d2d_s,)), (ici_in, (ici_s,))):
        for sem in sems:
            pltpu.make_async_copy(buf, buf, sem).wait()


def expand_kernel(len_ref, y_ref, out_hbm, buf, sem):
    tokens = out_hbm.shape[0]
    rows = y_ref.shape[3]
    seq_len = tokens // len_ref.shape[0]
    pos = lax.broadcasted_iota(jnp.int32, (tokens, rows), 1)
    place = (pos == row_targets(len_ref, (tokens, rows), 0, seq_len)).astype(jnp.bfloat16)
    steps, _, cols = buf.shape
    chunks = cols // CN

    def out_copy(i):
        return pltpu.make_async_copy(buf.at[i], out_hbm.at[:, pl.ds(i * cols, cols)], sem.at[i])

    for i in range(steps):
        wide = jnp.concatenate([y_ref[i * chunks + u, q // 2, q % 2] for u in range(chunks) for q in range(4)], axis=1)
        buf[i] = jnp.dot(place, wide, preferred_element_type=jnp.float32).astype(jnp.bfloat16)
        out_copy(i).start()
    for i in range(steps):
        out_copy(i).wait()


def solution(mesh):
    smem, hbm, vmem, anywhere = (pl.BlockSpec(memory_space=m) for m in (pltpu.SMEM, pltpu.HBM, pltpu.VMEM, pl.ANY))
    dma = lambda n: pltpu.SemaphoreType.DMA((n,))
    one = pltpu.SemaphoreType.DMA
    most = 208

    def with_rows(rows, have, w_loc, lengths):
        depth, width = w_loc.shape
        tokens = 256
        nc, nk = width // CN, depth // KB
        y = pl.pallas_call(
            main_kernel,
            out_shape=jax.ShapeDtypeStruct((nc, 2, 2, rows, 128), jnp.bfloat16),
            in_specs=[vmem, vmem, vmem, hbm],
            out_specs=anywhere,
            scratch_shapes=[
                pltpu.VMEM((SLOTS, KB, CN), jnp.bfloat16),
                pltpu.VMEM((nc, 2, 2, rows, 128), jnp.float32),
                pltpu.VMEM((nc, 2, rows, 128), jnp.float32),
                pltpu.VMEM((nc, rows, 128), jnp.float32),
                pltpu.VMEM((nc, rows, 128), jnp.bfloat16),
                pltpu.VMEM((nc, rows, 128), jnp.bfloat16),
                dma(SLOTS), one, dma(4), one, dma(RING), one, dma(RING), one, one, one, one, one, one],
            compiler_params=pltpu.CompilerParams(collective_id=1 + CAPS.index(rows), has_side_effects=True, vmem_limit_bytes=40 * 2**20),
            cost_estimate=pl.CostEstimate(flops=2 * rows * depth * width, bytes_accessed=2 * depth * width, transcendentals=0),
        )(*have, w_loc)
        steps = nc // 2
        return pl.pallas_call(
            expand_kernel,
            out_shape=pltpu.HBM((tokens, width), jnp.bfloat16),
            in_specs=[smem, vmem],
            out_specs=hbm,
            scratch_shapes=[pltpu.VMEM((steps, tokens, width // steps), jnp.bfloat16), dma(steps)],
            compiler_params=pltpu.CompilerParams(vmem_limit_bytes=16 * 2**20),
            cost_estimate=pl.CostEstimate(flops=2 * rows * tokens * width, bytes_accessed=4 * tokens * width, transcendentals=0),
        )(lengths, y)

    def local_part(x_loc, w_loc, lengths):
        tokens, depth = x_loc.shape
        nk = depth // KB
        groups = mesh.shape["data"]
        out_shape = [jax.ShapeDtypeStruct((1,), jnp.int32), pltpu.VMEM((most, depth), jnp.bfloat16),
                     pltpu.VMEM((FIRST, 2, 2, most, 128), jnp.float32), pltpu.VMEM((AHEAD, KB, CN), jnp.bfloat16)]
        scratch = [pltpu.VMEM((tokens, depth), jnp.bfloat16), pltpu.VMEM((8, 128), jnp.int32), pltpu.VMEM((groups - 1, 8, 128), jnp.int32),
                   dma(depth // XB), dma(groups - 1), dma(groups - 1),
                   pltpu.VMEM((FIRST * nk, KB, CN), jnp.bfloat16), dma(FIRST * nk), dma(AHEAD)]
        pick, *have = pl.pallas_call(
            head_kernel,
            out_shape=out_shape,
            in_specs=[smem, hbm, hbm],
            out_specs=[smem] + [vmem] * 3,
            scratch_shapes=scratch,
            compiler_params=pltpu.CompilerParams(collective_id=0, has_side_effects=True, vmem_limit_bytes=(12 + FIRST * 12) * 2**20),
            cost_estimate=pl.CostEstimate(flops=2 * most * depth * CN, bytes_accessed=2 * depth * CN, transcendentals=0),
        )(lengths, pltpu.with_memory_space_constraint(x_loc, pltpu.HBM), w_loc)
        return lax.switch(pick[0], [functools.partial(with_rows, cap) for cap in CAPS], have, w_loc, lengths)

    return jax.shard_map(local_part, mesh=mesh, in_specs=(P("data", "tp"), P("tp", None), P("data")), out_specs=P("data", None), check_vma=False)
```

```python
import functools

import jax
import jax.numpy as jnp
from jax import lax
from jax.experimental import pallas as pl
from jax.experimental.pallas import tpu as pltpu
from jax.sharding import PartitionSpec as P

MESH = pl.DeviceIdType.MESH
CAPS = (120, 128, 136, 144, 152, 160, 168, 176, 184, 200)
CN = 512
KB = 4096
XB = 4096
SLOTS = 6
FIRST = 1
AHEAD = 1
LAG_B, LAG_C, LAG_D = 1, 3, 5
RING = 8


def row_targets(len_ref, shape, axis, seq_len):
    row = lax.broadcasted_iota(jnp.int32, shape, axis)
    target = jnp.full(shape, -1, jnp.int32)
    start = jnp.int32(0)
    for s in range(len_ref.shape[0]):
        inside = (row >= s * seq_len) & (row < s * seq_len + len_ref[s])
        target = jnp.where(inside, row - s * seq_len + start, target)
        start = start + len_ref[s]
    return target


def head_kernel(len_ref, x_hbm, w_hbm, pick_ref, xc, *rest):
    part, ahead, x_buf, mine, theirs, x_sem, send, recv, w_buf, w_sem, a_sem = rest
    tokens, depth = x_hbm.shape
    rows = xc.shape[0]
    nk, nx = depth // KB, depth // XB
    seq_len = tokens // len_ref.shape[0]
    groups = theirs.shape[0] + 1
    me = lax.axis_index("data")
    peers = [{"data": lax.rem(me + r, groups)} for r in range(1, groups)]

    def x_copy(k):
        cols = pl.ds(pl.multiple_of(k * XB, XB), XB)
        return pltpu.make_async_copy(x_hbm.at[:, cols], x_buf.at[:, cols], x_sem.at[k])

    def w_copy(t):
        j, k = t // nk, t % nk
        return pltpu.make_async_copy(w_hbm.at[pl.ds(pl.multiple_of(k * KB, KB), KB), pl.ds(pl.multiple_of(j * CN, CN), CN)], w_buf.at[t], w_sem.at[t])

    def a_copy(k):
        return pltpu.make_async_copy(w_hbm.at[pl.ds(k * KB, KB), pl.ds(FIRST * CN, CN)], ahead.at[k], a_sem.at[k])

    def tell(r):
        return pltpu.make_async_remote_copy(src_ref=mine, dst_ref=theirs.at[r], send_sem=send.at[r], recv_sem=recv.at[r],
                                            device_id=peers[r], device_id_type=MESH)

    barrier = pltpu.get_barrier_semaphore()
    for dev in peers:
        pl.semaphore_signal(barrier, inc=1, device_id=dev, device_id_type=MESH)
    for k in range(nx):
        x_copy(k).start()
    for t in range(FIRST * nk):
        w_copy(t).start()
    for k in range(AHEAD):
        a_copy(k).start()
    total = len_ref[0]
    for s in range(1, len_ref.shape[0]):
        total = total + len_ref[s]
    mine[...] = jnp.full(mine.shape, total, jnp.int32)

    pos = lax.broadcasted_iota(jnp.int32, (rows, tokens), 0)
    pick = (pos == row_targets(len_ref, (rows, tokens), 1, seq_len)).astype(jnp.bfloat16)

    @pl.loop(0, nx)
    def _(k):
        x_copy(k).wait()
        cols = pl.ds(pl.multiple_of(k * XB, XB), XB)
        xc[:, cols] = jnp.dot(pick, x_buf[:, cols], preferred_element_type=jnp.float32).astype(jnp.bfloat16)

    pl.semaphore_wait(barrier, groups - 1)
    for r in range(groups - 1):
        tell(r).start()

    @pl.loop(0, FIRST * nk)
    def _(t):
        j, k = t // nk, lax.rem(t, nk)
        w_copy(t).wait()
        got = jnp.dot(xc[:, pl.ds(pl.multiple_of(k * KB, KB), KB)], w_buf[t], preferred_element_type=jnp.float32)
        for q in range(4):
            before = jnp.where(k == 0, 0.0, part[j, q // 2, q % 2])
            part[j, q // 2, q % 2] = before + got[:, q * 128:(q + 1) * 128]

    most = mine[...]
    for r in range(groups - 1):
        tell(r).wait()
        most = jnp.maximum(most, theirs[r])
    most = jnp.max(most)
    index = jnp.int32(0)
    for cap in CAPS[:-1]:
        index = index + (most > cap).astype(jnp.int32)
    pick_ref[0] = index
    for k in range(AHEAD):
        a_copy(k).wait()


def main_kernel(*refs):
    xc, first, ahead, w_hbm, y_out = refs[:5]
    (w_buf, part, d2d_in, ici_in, own, other, w_sem, d2d_s, d2d_r, ici_s, ici_r, yx_s, yx_r, yp_s, yp_r, yf_s, yf_r, yl_s, yo_s) = refs[5:]
    rows, depth = part.shape[3], xc.shape[1]
    width = w_hbm.shape[1]
    nc, nk = width // CN, depth // KB
    total = nc * nk
    tp = lax.axis_index("tp")
    me_x, me_c = tp // 2, lax.rem(tp, 2)
    nbr = {"tp": (1 - me_x) * 2 + me_c}
    partner = {"tp": me_x * 2 + (1 - me_c)}

    def w_copy(t, slot):
        j, k = t // nk, lax.rem(t, nk)
        return pltpu.make_async_copy(
            w_hbm.at[pl.ds(pl.multiple_of(k * KB, KB), KB), pl.ds(pl.multiple_of(j * CN, CN), CN)],
            w_buf.at[slot], w_sem.at[slot])

    barrier = pltpu.get_barrier_semaphore()
    for dev in (partner, nbr):
        pl.semaphore_signal(barrier, inc=1, device_id=dev, device_id_type=MESH)
    begin = FIRST * nk + AHEAD
    for t in range(begin, begin + SLOTS):
        w_copy(t, t % SLOTS).start()

    def remote(src, dst, s, r, dev):
        return pltpu.make_async_remote_copy(src_ref=src, dst_ref=dst, send_sem=s, recv_sem=r,
                                            device_id=dev, device_id_type=MESH)

    def d2d_copy(j):
        return remote(part.at[j, 1 - me_c], d2d_in.at[j], d2d_s, d2d_r.at[lax.rem(j, 4)], partner)

    def ici_copy(j):
        return remote(d2d_in.at[j, 1 - me_x], ici_in.at[j], ici_s, ici_r.at[lax.rem(j, RING)], nbr)

    def yx_copy(j):
        return remote(own.at[j], other.at[j], yx_s, yx_r.at[lax.rem(j, RING)], nbr)

    def yp_copy(j):
        return remote(own.at[j], y_out.at[j, me_c, me_x], yp_s, yp_r, partner)

    def yf_copy(j):
        return remote(other.at[j], y_out.at[j, me_c, 1 - me_x], yf_s, yf_r, partner)

    def yl_copy(j):
        return pltpu.make_async_copy(own.at[j], y_out.at[j, me_c, me_x], yl_s)

    def yo_copy(j):
        return pltpu.make_async_copy(other.at[j], y_out.at[j, me_c, 1 - me_x], yo_s)

    def stage_a(j):
        d2d_copy(j).start()

    def stage_b(j):
        d2d_copy(j).wait_recv()
        d2d_in[j, 1 - me_x] = d2d_in[j, 1 - me_x] + part[j, me_c, 1 - me_x]
        d2d_in[j, me_x] = d2d_in[j, me_x] + part[j, me_c, me_x]
        ici_copy(j).start()

    def stage_c(j):
        ici_copy(j).wait_recv()
        own[j] = (d2d_in[j, me_x] + ici_in[j]).astype(jnp.bfloat16)
        yx_copy(j).start()
        yp_copy(j).start()
        yl_copy(j).start()

    def stage_d(j):
        yx_copy(j).wait_recv()
        yf_copy(j).start()
        yo_copy(j).start()

    def when_valid(j, stage, least=0):
        @pl.when((j >= least) & (j < nc))
        def _():
            stage(j)

    for j in range(FIRST):
        for q in range(4):
            part[j, q // 2, q % 2] = first[j, q // 2, q % 2, :rows]
    pl.semaphore_wait(barrier, 2)
    for j in range(FIRST):
        stage_a(j)
        stage_b(j)

    def multiply(w, j, k):
        got = jnp.dot(xc[:rows, pl.ds(pl.multiple_of(k * KB, KB), KB)], w[...], preferred_element_type=jnp.float32)
        for q in range(4):
            before = jnp.where(k == 0, 0.0, part[j, q // 2, q % 2])
            part[j, q // 2, q % 2] = before + got[:, q * 128:(q + 1) * 128]

    @pl.loop(0, AHEAD)
    def _(k):
        multiply(ahead.at[k], FIRST, k)

    @pl.loop(begin, (nc + LAG_D) * nk)
    def _(t):
        j, k = t // nk, lax.rem(t, nk)

        @pl.when(t < total)
        def _():
            slot = lax.rem(t, SLOTS)
            w_copy(t, slot).wait()
            multiply(w_buf.at[slot], j, k)

            @pl.when(t + SLOTS < total)
            def _():
                w_copy(t + SLOTS, slot).start()

        @pl.when(k == 0)
        def _():
            when_valid(j - LAG_B, stage_b, FIRST)
            when_valid(j - LAG_C, stage_c)

        @pl.when(k == nk - 1)
        def _():
            when_valid(j, stage_a)
            when_valid(j - LAG_D, stage_d)

    for buf, sems in ((own, (yp_r, yf_r, yl_s, yo_s, yx_s, yp_s, yf_s)), (d2d_in, (d2d_s,)), (ici_in, (ici_s,))):
        for sem in sems:
            pltpu.make_async_copy(buf, buf, sem).wait()


def expand_kernel(len_ref, y_ref, out_hbm, buf, sem):
    tokens = out_hbm.shape[0]
    rows = y_ref.shape[3]
    seq_len = tokens // len_ref.shape[0]
    pos = lax.broadcasted_iota(jnp.int32, (tokens, rows), 1)
    place = (pos == row_targets(len_ref, (tokens, rows), 0, seq_len)).astype(jnp.bfloat16)
    steps, _, cols = buf.shape
    chunks = cols // CN

    def out_copy(i):
        return pltpu.make_async_copy(buf.at[i], out_hbm.at[:, pl.ds(i * cols, cols)], sem.at[i])

    for i in range(steps):
        wide = jnp.concatenate([y_ref[i * chunks + u, q // 2, q % 2] for u in range(chunks) for q in range(4)], axis=1)
        buf[i] = jnp.dot(place, wide, preferred_element_type=jnp.float32).astype(jnp.bfloat16)
        out_copy(i).start()
    for i in range(steps):
        out_copy(i).wait()


def solution(mesh):
    smem, hbm, vmem, anywhere = (pl.BlockSpec(memory_space=m) for m in (pltpu.SMEM, pltpu.HBM, pltpu.VMEM, pl.ANY))
    dma = lambda n: pltpu.SemaphoreType.DMA((n,))
    one = pltpu.SemaphoreType.DMA
    most = 208

    def with_rows(rows, have, w_loc, lengths):
        depth, width = w_loc.shape
        tokens = 256
        nc, nk = width // CN, depth // KB
        y = pl.pallas_call(
            main_kernel,
            out_shape=jax.ShapeDtypeStruct((nc, 2, 2, rows, 128), jnp.bfloat16),
            in_specs=[vmem, vmem, vmem, hbm],
            out_specs=anywhere,
            scratch_shapes=[
                pltpu.VMEM((SLOTS, KB, CN), jnp.bfloat16),
                pltpu.VMEM((nc, 2, 2, rows, 128), jnp.float32),
                pltpu.VMEM((nc, 2, rows, 128), jnp.float32),
                pltpu.VMEM((nc, rows, 128), jnp.float32),
                pltpu.VMEM((nc, rows, 128), jnp.bfloat16),
                pltpu.VMEM((nc, rows, 128), jnp.bfloat16),
                dma(SLOTS), one, dma(4), one, dma(RING), one, dma(RING), one, one, one, one, one, one],
            compiler_params=pltpu.CompilerParams(collective_id=1 + CAPS.index(rows), has_side_effects=True, vmem_limit_bytes=40 * 2**20),
            cost_estimate=pl.CostEstimate(flops=2 * rows * depth * width, bytes_accessed=2 * depth * width, transcendentals=0),
        )(*have, w_loc)
        steps = nc // 2
        return pl.pallas_call(
            expand_kernel,
            out_shape=pltpu.HBM((tokens, width), jnp.bfloat16),
            in_specs=[smem, vmem],
            out_specs=hbm,
            scratch_shapes=[pltpu.VMEM((steps, tokens, width // steps), jnp.bfloat16), dma(steps)],
            compiler_params=pltpu.CompilerParams(vmem_limit_bytes=16 * 2**20),
            cost_estimate=pl.CostEstimate(flops=2 * rows * tokens * width, bytes_accessed=4 * tokens * width, transcendentals=0),
        )(lengths, y)

    def local_part(x_loc, w_loc, lengths):
        tokens, depth = x_loc.shape
        nk = depth // KB
        groups = mesh.shape["data"]
        out_shape = [jax.ShapeDtypeStruct((1,), jnp.int32), pltpu.VMEM((most, depth), jnp.bfloat16),
                     pltpu.VMEM((FIRST, 2, 2, most, 128), jnp.float32), pltpu.VMEM((AHEAD, KB, CN), jnp.bfloat16)]
        scratch = [pltpu.VMEM((tokens, depth), jnp.bfloat16), pltpu.VMEM((8, 128), jnp.int32), pltpu.VMEM((groups - 1, 8, 128), jnp.int32),
                   dma(depth // XB), dma(groups - 1), dma(groups - 1),
                   pltpu.VMEM((FIRST * nk, KB, CN), jnp.bfloat16), dma(FIRST * nk), dma(AHEAD)]
        pick, *have = pl.pallas_call(
            head_kernel,
            out_shape=out_shape,
            in_specs=[smem, hbm, hbm],
            out_specs=[smem] + [vmem] * 3,
            scratch_shapes=scratch,
            compiler_params=pltpu.CompilerParams(collective_id=0, has_side_effects=True, vmem_limit_bytes=(12 + FIRST * 12) * 2**20),
            cost_estimate=pl.CostEstimate(flops=2 * most * depth * CN, bytes_accessed=2 * depth * CN, transcendentals=0),
        )(lengths, pltpu.with_memory_space_constraint(x_loc, pltpu.HBM), w_loc)
        return lax.switch(pick[0], [functools.partial(with_rows, cap) for cap in CAPS], have, w_loc, lengths)

    return jax.shard_map(local_part, mesh=mesh, in_specs=(P("data", "tp"), P("tp", None), P("data")), out_specs=P("data", None), check_vma=False)
```
